32 devices in a mesh: blk: 32 (over z, y, x, core).
Axes of the slice: x: 2, y: 2, z: 4, core: 2. Of those that a mesh axis runs over, the one named last changes fastest.
Arguments:
- single: bfloat16 [512, 384], P('blk'), may hold values from -6 to 6
- angles: float32 [3, 512], P(None, 'blk'), may hold values from -3.140625 to 3.140625
- trans: float32 [3, 512], P(None, 'blk'), may hold values from -6 to 6
- left_factor: bfloat16 [512, 64], P('blk'), may hold values from -6 to 6
- right_factor: bfloat16 [512, 64], P('blk'), may hold values from -6 to 6
- chain: int32 [512], P('blk'), may hold values from 0 to 7, never falling along the last dimension, each value on 1 to 128 neighbouring positions
- live: int32 [512], P('blk'), may hold values 0 or 1
- w_query: bfloat16 [384, 192], replicated, may hold values from -0.3125 to 0.3125
- w_keyval: bfloat16 [384, 384], replicated, may hold values from -0.3125 to 0.3125
- w_qpoints: bfloat16 [384, 144], replicated, may hold values from -0.3125 to 0.3125
- w_kvpoints: bfloat16 [384, 432], replicated, may hold values from -0.3125 to 0.3125
- w_pair_in: bfloat16 [64, 128], replicated, may hold values from -0.75 to 0.75
- chain_bias: float32 [128], replicated, may hold values from -6 to 6
- w_pair_out: bfloat16 [128, 128], replicated, may hold values from -0.5 to 0.5
- w_bias: bfloat16 [128, 12], replicated, may hold values from -0.5 to 0.5
- point_weight: float32 [12], replicated, may hold values from 0.1 to 1
- w_out: bfloat16 [2112, 384], replicated, may hold values from -0.125 to 0.125
- out_gain: float32 [384], replicated, may hold values from 0.5 to 1.5
- w_frame: float32 [384, 6], replicated, may hold values from -0.3125 to 0.3125
Outputs:
- single_out: bfloat16 [512, 384], P('blk')
- frames_out: float32 [12, 512], P(None, 'blk')
The draws below stay inside these ranges and needn't reach their ends.
Inputs may be any that keep to these rules, and one draw needn't show every extreme that they name: Residues of one chain are consecutive and chain numbers never fall along the residues; a chain has 1 to 128 residues.
All inputs are finite; a program needn't handle non-finite values. No bound on the sum of `live` on one device may be relied on, other than what follows from the above.
Results may differ from the reference program's by a relative error of at most 0.0035.
Values may be sent and summed in bfloat16 or wider, within the bound.
A program may use at most 192 MiB of HBM per device.

```python
import math
import jax
import jax.numpy as jnp
import numpy as np
from jax import lax

CS = 384
HEADS = 12
HEAD_DIM = 16
QPTS = 4
VPTS = 8
CZ = 128
RANK = 64
CHAINS = 8
RES_DEV = 16
RES = 512
N_BLK = 32


def place_ends(result, rng, smallest, largest):
    index_at = [jax.random.randint(jax.random.fold_in(rng, axis), (), 0, length) for axis, length in enumerate(result.shape)]
    main_axis = result.shape.index(max(result.shape))
    beside = index_at[:main_axis] + [(index_at[main_axis] + 1) % result.shape[main_axis]] + index_at[main_axis + 1:]
    return result.at[tuple(index_at)].set(smallest).at[tuple(beside)].set(largest)


def block_levels(stream_key, shape, split, smallest, top_value):
    level = 1.0
    for position, blocks in split:
        draws = jax.random.uniform(jax.random.fold_in(jax.random.fold_in(stream_key, 6), position), (blocks,), jnp.float32, smallest / len(split), top_value / len(split))
        level = level * jnp.repeat(jnp.exp(draws), shape[position] // blocks).reshape((-1,) + (1,) * (len(shape) - 1 - position))
    return level


def length_profile(amount, total, bound, skew):
    portions = [(1 << 20) // math.isqrt(standing ** skew) + 1 for standing in range(2, amount + 1)]
    rest, given = total - bound - (amount - 1), [1] * (amount - 1)
    while rest > 0:
        free = [i for i in range(amount - 1) if given[i] < bound]
        pool, remaining = sum([portions[i] for i in free]), rest
        for i in free:
            more = min(bound - given[i], max(1, remaining * portions[i] // pool), rest)
            given[i] = given[i] + more
            rest = rest - more
    return np.array([bound] + given)


def ragged_sizes(stream_key, amount, total, reach, slope):
    if amount == 2:
        one = jax.random.randint(stream_key, (), max(1, total - reach), min(reach, total - 1) + 1)
        return jnp.stack([one, total - one])
    sizes = jnp.asarray(length_profile(amount, total, reach, slope), jnp.int32)
    twos = (amount - 1) // 2
    source_of, taker = sizes[1:1 + 2 * twos:2], sizes[2:2 + 2 * twos:2]
    slack = jnp.minimum(source_of - 1, reach - taker)
    moved = jax.random.randint(jax.random.fold_in(stream_key, 1), (twos,), 0, 1 << 20) % (slack + 1)
    sizes = sizes.at[1:1 + 2 * twos:2].set(source_of - moved).at[2:2 + 2 * twos:2].set(taker + moved)
    return sizes[jax.random.permutation(jax.random.fold_in(stream_key, 2), amount)]


def bell_draw(key, shape, scale, limit, split=(), kind=jnp.bfloat16):
    entries = jax.random.normal(key, shape, jnp.float32) * scale
    if len(split) > 0:
        entries = block_levels(key, shape, split, -0.22, 0.18) * entries
    return jnp.clip(entries, min=-limit, max=limit).astype(kind)


def setup_inputs(seed: int = 0) -> dict:
    streams_of = jax.random.split(jax.random.key(seed), 20)
    return {
        "single": bell_draw(streams_of[0], (RES, CS), 1.0, 6.0, ((0, 32),)),
        "angles": jnp.clip(jax.random.uniform(streams_of[1], (3, RES), jnp.float32, -3.140625, 3.140625), -3.140625, 3.140625),
        "trans": bell_draw(streams_of[2], (3, RES), 1.0, 6.0, ((1, 32),), jnp.float32),
        "left_factor": bell_draw(streams_of[3], (RES, RANK), 1.0, 6.0, ((0, 32),)),
        "right_factor": bell_draw(streams_of[4], (RES, RANK), 1.0, 6.0, ((0, 32),)),
        "chain": jnp.searchsorted(jnp.cumsum(ragged_sizes(streams_of[5], CHAINS, RES, RES // 4, 0)), jnp.arange(RES), side="right").astype(jnp.int32),
        "live": place_ends((jax.random.randint(streams_of[6], (RES,), 0, 16) < 15).astype(jnp.int32), jax.random.fold_in(streams_of[6], 1), 0, 1),
        "w_query": bell_draw(streams_of[7], (CS, HEADS * HEAD_DIM), CS ** -0.5, 0.3125),
        "w_keyval": bell_draw(streams_of[8], (CS, 2 * HEADS * HEAD_DIM), CS ** -0.5, 0.3125),
        "w_qpoints": bell_draw(streams_of[9], (CS, 3 * HEADS * QPTS), CS ** -0.5, 0.3125),
        "w_kvpoints": bell_draw(streams_of[10], (CS, 3 * HEADS * (QPTS + VPTS)), CS ** -0.5, 0.3125),
        "w_pair_in": bell_draw(streams_of[11], (RANK, CZ), RANK ** -0.5, 0.75),
        "chain_bias": bell_draw(streams_of[12], (CZ,), 1.0, 6.0, (), jnp.float32),
        "w_pair_out": bell_draw(streams_of[13], (CZ, CZ), CZ ** -0.5, 0.5),
        "w_bias": bell_draw(streams_of[14], (CZ, HEADS), CZ ** -0.5, 0.5),
        "point_weight": jnp.clip(jnp.exp(jax.random.uniform(streams_of[15], (HEADS,), jnp.float32, math.log(0.1), math.log(1.0))), 0.1, 1.0),
        "w_out": bell_draw(streams_of[16], (HEADS * (HEAD_DIM + 4 * VPTS + CZ), CS), (HEADS * (HEAD_DIM + 4 * VPTS + CZ)) ** -0.5, 0.125),
        "out_gain": jnp.clip(1.0 + 0.1 * jax.random.normal(streams_of[17], (CS,), jnp.float32), 0.5, 1.5),
        "w_frame": bell_draw(streams_of[18], (CS, 6), CS ** -0.5, 0.3125, (), jnp.float32),
    }


def mm(form, left, right):
    return jnp.einsum(form, left.astype(jnp.float32), right.astype(jnp.float32), precision=lax.Precision.HIGHEST)

def rotation(angles):
    ca, sa = (jnp.cos(angles[0]), jnp.sin(angles[0]))
    cb, sb = (jnp.cos(angles[1]), jnp.sin(angles[1]))
    cc, sc = (jnp.cos(angles[2]), jnp.sin(angles[2]))
    first = jnp.stack([ca * cb, -sa * cc + ca * sb * sc, sa * sc + ca * sb * cc])
    second = jnp.stack([sa * cb, ca * cc + sa * sb * sc, -ca * sc + sa * sb * cc])
    third = jnp.stack([-sb, cb * sc, cb * cc])
    return jnp.stack([first, second, third])

def quat_rotation(bpart, cpart, dpart):
    norm = jnp.sqrt(1.0 + bpart * bpart + cpart * cpart + dpart * dpart)
    apart = 1.0 / norm
    bpart, cpart, dpart = (bpart / norm, cpart / norm, dpart / norm)
    first = jnp.stack([apart * apart + bpart * bpart - cpart * cpart - dpart * dpart, 2.0 * (bpart * cpart - apart * dpart), 2.0 * (bpart * dpart + apart * cpart)])
    second = jnp.stack([2.0 * (bpart * cpart + apart * dpart), apart * apart - bpart * bpart + cpart * cpart - dpart * dpart, 2.0 * (cpart * dpart - apart * bpart)])
    third = jnp.stack([2.0 * (bpart * dpart - apart * cpart), 2.0 * (cpart * dpart + apart * bpart), apart * apart - bpart * bpart - cpart * cpart + dpart * dpart])
    return jnp.stack([first, second, third])

def to_global(rot, shift, points):
    return jnp.einsum('xyn,nyhp->nxhp', rot, points, precision=lax.Precision.HIGHEST) + shift.T[:, :, None, None]

def pair_features(left, right, same, w_pair_in, chain_bias, w_pair_out):
    prod = (left.astype(jnp.float32)[:, None, :] * right.astype(jnp.float32)[None, :, :]).astype(jnp.bfloat16)
    hidden = mm('qkr,rz->qkz', prod, w_pair_in) + same[:, :, None] * chain_bias
    hidden = jax.nn.gelu(hidden, approximate=True).astype(jnp.bfloat16)
    outer = mm('qkz,zy->qky', hidden, w_pair_out)
    center = outer - lax.optimization_barrier(jnp.mean(outer, axis=2, keepdims=True))
    spread = lax.optimization_barrier(jnp.mean(center * center, axis=2, keepdims=True))
    return (center * lax.rsqrt(spread + 1e-05)).astype(jnp.bfloat16)

def reference(single, angles, trans, left_factor, right_factor, chain, live, w_query, w_keyval, w_qpoints, w_kvpoints, w_pair_in, chain_bias, w_pair_out, w_bias, point_weight, w_out, out_gain, w_frame):
    width = HEADS * HEAD_DIM
    rot = rotation(angles)
    keyval = jnp.dot(single, w_keyval, preferred_element_type=jnp.float32).astype(jnp.bfloat16)
    keys = keyval[:, :width].reshape(RES, HEADS, HEAD_DIM)
    values = keyval[:, width:].reshape(RES, HEADS, HEAD_DIM)
    kvpoints = jnp.dot(single, w_kvpoints, preferred_element_type=jnp.float32).reshape(RES, 3, HEADS, QPTS + VPTS)
    kvglobal = to_global(rot, trans, kvpoints).astype(jnp.bfloat16)
    kglobal = kvglobal[..., :QPTS].astype(jnp.float32)
    vglobal = kvglobal[..., QPTS:]
    ksq = lax.optimization_barrier(jnp.sum(kglobal * kglobal, axis=(1, 3))).T
    coef = point_weight * (2.0 / (9.0 * QPTS)) ** 0.5 / 2.0
    dead = 100000.0 * (1.0 - live.astype(jnp.float32))

    def one_block(index):
        start = index * RES_DEV
        rows = lax.dynamic_slice_in_dim(single, start, RES_DEV, 0)
        rot_rows = lax.dynamic_slice_in_dim(rot, start, RES_DEV, 2)
        trans_rows = lax.dynamic_slice_in_dim(trans, start, RES_DEV, 1)
        left_rows = lax.dynamic_slice_in_dim(left_factor, start, RES_DEV, 0)
        chain_rows = lax.dynamic_slice_in_dim(chain, start, RES_DEV, 0)
        query = jnp.dot(rows, w_query, preferred_element_type=jnp.float32).astype(jnp.bfloat16).reshape(RES_DEV, HEADS, HEAD_DIM)
        qpoints = jnp.dot(rows, w_qpoints, preferred_element_type=jnp.float32).reshape(RES_DEV, 3, HEADS, QPTS)
        qglobal = to_global(rot_rows, trans_rows, qpoints)
        qsq = lax.optimization_barrier(jnp.sum(qglobal * qglobal, axis=(1, 3))).T
        same = (chain_rows[:, None] == chain[None, :]).astype(jnp.float32)
        pair = pair_features(left_rows, right_factor, same, w_pair_in, chain_bias, w_pair_out)
        scalar = mm('qhc,khc->hqk', query, keys) * HEAD_DIM ** (-0.5)
        bias = mm('qkz,zh->hqk', pair, w_bias)
        cross = mm('qxhp,kxhp->hqk', qglobal, kglobal)
        dist = qsq[:, :, None] + ksq[:, None, :] - 2.0 * cross
        logits = (1.0 / 3.0) ** 0.5 * (scalar + bias - coef[:, None, None] * dist) - dead[None, None, :]
        top = lax.optimization_barrier(jnp.max(logits, axis=2, keepdims=True))
        terms = jnp.exp(logits - top)
        total = lax.optimization_barrier(jnp.sum(terms, axis=2))
        weights = terms.astype(jnp.bfloat16)
        att_values = mm('hqk,khc->hqc', weights, values) / total[:, :, None]
        att_points = mm('hqk,kxhp->hqxp', weights, vglobal) / total[:, :, None, None]
        att_pair = mm('hqk,qkz->hqz', weights, pair) / total[:, :, None]
        local = jnp.einsum('yxq,hqyp->hqxp', rot_rows, att_points - trans_rows.T[None, :, :, None], precision=lax.Precision.HIGHEST)
        pnorm = jnp.sqrt(lax.optimization_barrier(jnp.sum(local * local, axis=2)) + 1e-08)
        return jnp.concatenate([att_values.transpose(1, 0, 2).reshape(RES_DEV, -1), local.transpose(1, 2, 0, 3).reshape(RES_DEV, -1), pnorm.transpose(1, 0, 2).reshape(RES_DEV, -1), att_pair.transpose(1, 0, 2).reshape(RES_DEV, -1)], axis=1).astype(jnp.bfloat16)
    features = lax.map(one_block, jnp.arange(N_BLK, dtype=jnp.int32) * 1).reshape(RES, -1)
    mixed = jnp.dot(features, w_out, preferred_element_type=jnp.float32) + single.astype(jnp.float32)
    center = mixed - lax.optimization_barrier(jnp.mean(mixed, axis=1, keepdims=True))
    snew = center * lax.rsqrt(lax.optimization_barrier(jnp.mean(center * center, axis=1, keepdims=True)) + 1e-05) * out_gain
    update = jnp.dot(snew, w_frame, precision=lax.Precision.HIGHEST)
    upd_rot = quat_rotation(update[:, 0], update[:, 1], update[:, 2])
    new_rot = jnp.einsum('xyn,yzn->xzn', rot, upd_rot, precision=lax.Precision.HIGHEST)
    new_trans = jnp.einsum('xyn,yn->xn', rot, update[:, 3:].T, precision=lax.Precision.HIGHEST) + trans
    frames_out = jnp.concatenate([new_rot.reshape(9, RES), new_trans], axis=0)
    return (snew.astype(jnp.bfloat16), frames_out)
```

```python
import functools

import jax
import jax.numpy as jnp
from jax import lax
from jax.experimental import pallas as pl
from jax.experimental.pallas import tpu as pltpu
from jax.sharding import PartitionSpec as P

F32 = jnp.float32
BF16 = jnp.bfloat16
MESH = pl.DeviceIdType.MESH
HP = 16
CHAINS = 8
AUX = 128


def rotation(angles):
    ca, sa = (jnp.cos(angles[0]), jnp.sin(angles[0]))
    cb, sb = (jnp.cos(angles[1]), jnp.sin(angles[1]))
    cc, sc = (jnp.cos(angles[2]), jnp.sin(angles[2]))
    return [
        ca * cb, -sa * cc + ca * sb * sc, sa * sc + ca * sb * cc,
        sa * cb, ca * cc + sa * sb * sc, -ca * sc + sa * sb * cc,
        -sb, cb * sc, cb * cc,
    ]


def dot(a, b):
    return jnp.dot(a, b, preferred_element_type=F32)


def dot_t(a, b):
    return lax.dot_general(a, b, (((1,), (1,)), ((), ())), preferred_element_type=F32)


def split3(x):
    hi = x.astype(BF16)
    rest = x - hi.astype(F32)
    mid = rest.astype(BF16)
    lo = (rest - mid.astype(F32)).astype(BF16)
    return hi, mid, lo


def onehot(mask):
    return jnp.where(mask, 1.0, 0.0).astype(BF16)


def iota(shape, dim):
    return lax.broadcasted_iota(jnp.int32, shape, dim)


def frame_columns(aux, base):
    wide = aux.astype(F32)
    return (
        wide[:, base : base + 12] + wide[:, base + 12 : base + 24] + wide[:, base + 24 : base + 36]
    )


def kernel(
    n, dims, payload, left, coef_in, w_pair_in, chain_bias, w_pair_out, w_bias, out_gain, w_frame,
    w_query_h, w_keyval_h, w_qpoints_h, w_kvpoints_h, w_out_h,
    single_out, frames_out,
    gat, w_query, w_keyval, w_qpoints, w_kvpoints, w_out, kv, kg, logit, wts, pair, attp, scale,
    win2, wout2, dead,
    send_sem, recv_sem, relay_sem, own_sem, w_sem,
):
    heads, head_dim, qpts, vpts, rank, pair_dim = dims
    rows, cs = single_out.shape
    keys = n * rows
    width = heads * head_dim
    pts = qpts + vpts
    pw = heads * pts
    fbase = rank + 3 * CHAINS
    third = (1.0 / 3.0) ** 0.5
    me = lax.axis_index("blk")
    chips = n // 2
    core = me % 2
    chip = me // 2
    sib = chip * 2 + 1 - core

    loads = [
        pltpu.make_async_copy(src, dst, w_sem.at[i])
        for i, (src, dst) in enumerate(
            [
                (w_query_h, w_query),
                (w_qpoints_h, w_qpoints),
                (w_keyval_h, w_keyval),
                (w_kvpoints_h, w_kvpoints),
                (w_out_h, w_out),
            ]
        )
    ]
    barrier = pltpu.get_barrier_semaphore()

    def peer_of(d):
        return ((chip + d) % chips) * 2 + core

    def block(dev):
        return gat.at[pl.ds(pl.multiple_of(dev * rows, rows), rows), :]

    @pl.loop(1, chips)
    def _(d):
        pl.semaphore_signal(barrier, inc=1, device_id=(peer_of(d),), device_id_type=MESH)

    pl.semaphore_signal(barrier, inc=1, device_id=(sib,), device_id_type=MESH)
    own = pltpu.make_async_copy(payload, block(me), own_sem)
    own.start()
    for item in loads:
        item.start()
    pl.semaphore_wait(barrier, chips)

    def send(dev):
        return pltpu.make_async_remote_copy(
            src_ref=payload, dst_ref=block(me), send_sem=send_sem.at[dev], recv_sem=recv_sem.at[me],
            device_id=(dev,), device_id_type=MESH,
        )

    def arrival(dev):
        return pltpu.make_async_remote_copy(
            src_ref=payload, dst_ref=block(dev), send_sem=send_sem.at[dev],
            recv_sem=recv_sem.at[dev], device_id=(sib,), device_id_type=MESH,
        )

    def relay(dev):
        return pltpu.make_async_remote_copy(
            src_ref=block(dev), dst_ref=block(dev), send_sem=relay_sem.at[dev],
            recv_sem=recv_sem.at[dev], device_id=(sib,), device_id_type=MESH,
        )

    @pl.loop(1, chips)
    def _(d):
        send(peer_of(d)).start()

    send(sib).start()

    own_x = payload[:, :cs]
    own_frame = frame_columns(payload[:, cs:], fbase)
    loads[0].wait()
    loads[1].wait()
    query = dot(own_x, w_query[...]).astype(BF16).astype(F32)
    hrow = iota((rows, HP, width), 1)
    lane = iota((rows, HP, width), 2)
    vmask = ((lane >= hrow * head_dim) & (lane < (hrow + 1) * head_dim)).reshape(rows * HP, width)
    a_query = jnp.where(
        vmask, jnp.broadcast_to(query[:, None, :], (rows, HP, width)).reshape(rows * HP, width), 0.0
    ).astype(BF16)
    part = heads * qpts
    spread = jnp.where(
        (iota((part, pw), 0) // qpts) * pts + iota((part, pw), 0) % qpts == iota((part, pw), 1), 1.0, 0.0
    ).astype(BF16)
    qp = [
        dot(own_x, dot(w_qpoints[:, y * part : (y + 1) * part], spread).astype(BF16))
        for y in range(3)
    ]
    hrow = iota((rows, HP, pw), 1)
    lane = iota((rows, HP, pw), 2)
    kmask = ((lane >= hrow * pts) & (lane < hrow * pts + qpts)).reshape(rows * HP, pw)
    amask = ((lane >= hrow * pts) & (lane < (hrow + 1) * pts)).reshape(rows * HP, pw)
    a_points = []
    qsum = 0.0
    for x in range(3):
        point = own_frame[:, 9 + x : 10 + x]
        for y in range(3):
            point = point + own_frame[:, 3 * x + y : 3 * x + y + 1] * qp[y]
        a_x = jnp.where(
            kmask, jnp.broadcast_to(point[:, None, :], (rows, HP, pw)).reshape(rows * HP, pw), 0.0
        )
        qsum = qsum + a_x * a_x
        a_points.append(split3(a_x))
    qsq = jnp.sum(qsum, axis=1, keepdims=True)
    coef16 = coef_in[...]
    coef = jnp.broadcast_to(coef16[None], (rows, HP, 1)).reshape(rows * HP, 1)

    bias_parts = [
        jnp.broadcast_to(item.astype(F32), (CHAINS, pair_dim)) for item in split3(chain_bias[...])
    ]
    w_in = jnp.concatenate(
        [w_pair_in[...].astype(F32)] + bias_parts + [jnp.zeros((AUX - fbase, pair_dim), F32)], axis=0
    ).astype(BF16)
    none = jnp.zeros((pair_dim, pair_dim), BF16)
    win2[...] = jnp.concatenate(
        [jnp.concatenate([w_in, none], axis=1), jnp.concatenate([none, w_in], axis=1)], axis=0
    )
    w_o = w_pair_out[...]
    wout2[...] = jnp.concatenate(
        [jnp.concatenate([w_o, none], axis=1), jnp.concatenate([none, w_o], axis=1)], axis=0
    )
    eye = onehot(iota((HP, heads), 0) == iota((HP, heads), 1))
    w_b = dot_t(eye, w_bias[...]).astype(BF16)
    none = jnp.zeros((HP, pair_dim), BF16)
    w_b2 = jnp.concatenate(
        [jnp.concatenate([w_b, none], axis=1), jnp.concatenate([none, w_b], axis=1)], axis=0
    )

    @pl.loop(1, chips)
    def _(d):
        dev = peer_of(d)
        arrival(dev).wait_recv()
        relay(dev).start()

    own.wait()
    loads[2].wait()
    loads[3].wait()
    arrival(sib).wait_recv()

    @pl.loop(1, chips)
    def _(d):
        arrival(((chip + d) % chips) * 2 + 1 - core).wait_recv()

    kb = 128
    hrow = iota((HP, pw), 0)
    lane = iota((HP, pw), 1)
    hsel = onehot((lane >= hrow * pts) & (lane < hrow * pts + qpts))
    live_sel = onehot(iota((HP, AUX), 1) == fbase + 36)

    @pl.loop(0, keys // kb)
    def _(b):
        at = pl.ds(pl.multiple_of(b * kb, kb), kb)
        x_in = gat[at, :cs]
        aux = gat[at, cs:]
        keyval = dot(x_in, w_keyval[...]).astype(BF16)
        kv[at, :] = keyval
        kp = dot(x_in, w_kvpoints[...])
        frame = frame_columns(aux, fbase)
        scalar = dot_t(a_query, keyval[:, :width]) * head_dim ** (-0.5)
        cross = 0.0
        square = 0.0
        for x in range(3):
            point = frame[:, 9 + x : 10 + x]
            for y in range(3):
                point = point + frame[:, 3 * x + y : 3 * x + y + 1] * kp[:, y * pw : (y + 1) * pw]
            point = point.astype(BF16)
            kg[x, at, :] = point
            wide = point.astype(F32)
            square = square + wide * wide
            for item in a_points[x]:
                cross = cross + dot_t(item, point)
        ksq = 0.0
        for item in split3(square):
            ksq = ksq + dot_t(hsel, item)
        ksq = jnp.broadcast_to(ksq[None], (rows, HP, kb)).reshape(rows * HP, kb)
        logit[:, at] = scalar - coef * (qsq + ksq - 2.0 * cross)
        dead[:, at] = 100000.0 * (1.0 - dot_t(live_sel, aux))

    @pl.loop(0, rows // 2)
    def _(t):
        left0 = left[pl.ds(2 * t, 1), :]
        left1 = left[pl.ds(2 * t + 1, 1), :]

        @pl.loop(0, keys // kb, unroll=2)
        def _(b):
            at = pl.ds(pl.multiple_of(b * kb, kb), kb)
            right = gat[at, cs:].astype(F32)
            prod = jnp.concatenate(
                [(right * left0).astype(BF16), (right * left1).astype(BF16)], axis=1
            )
            hidden = dot(prod, win2[...])
            hidden = jax.nn.gelu(hidden, approximate=True).astype(BF16)
            outer = dot(hidden, wout2[...])
            for half in range(2):
                o = outer[:, half * pair_dim : (half + 1) * pair_dim]
                center = o - jnp.mean(o, axis=1, keepdims=True)
                var = jnp.mean(center * center, axis=1, keepdims=True)
                pair[at, half * pair_dim : (half + 1) * pair_dim] = (
                    center * lax.rsqrt(var + 1e-05)
                ).astype(BF16)

        sel = pl.ds(pl.multiple_of(t * 2 * HP, 2 * HP), 2 * HP)
        both = pair[...]
        bias = dot_t(w_b2, both)
        row = third * (logit[sel, :] + bias) - jnp.concatenate([dead[...], dead[...]], axis=0)
        top = jnp.max(row, axis=1, keepdims=True)
        terms = jnp.exp(row - top)
        inv = 1.0 / jnp.sum(terms, axis=1, keepdims=True)
        weight = terms.astype(BF16)
        wts[sel, :] = weight
        scale[sel, :] = jnp.broadcast_to(inv, (2 * HP, 128))
        out = dot(weight, both) * inv
        attp[sel, :] = jnp.concatenate([out[:HP, :pair_dim], out[HP:, pair_dim:]], axis=0)

    weight = wts[...]
    inv = scale[:, :1]

    def pick(value, mask):
        value = jnp.where(mask, value * inv, 0.0)
        return jnp.sum(value.reshape(rows, HP, value.shape[1]), axis=1)

    values = pick(dot(weight, kv[:, width:]), vmask)
    away = [
        pick(dot(weight, kg[y]), amask) - own_frame[:, 9 + y : 10 + y] for y in range(3)
    ]
    out_cols = heads * vpts
    narrow = jnp.where(
        iota((pw, out_cols), 0)
        == (iota((pw, out_cols), 1) // vpts) * pts + qpts + iota((pw, out_cols), 1) % vpts,
        1.0, 0.0,
    ).astype(BF16)
    loads[4].wait()
    mixed = own_x.astype(F32) + dot(values.astype(BF16), w_out[:width, :])
    norm = 0.0
    for x in range(3):
        local = 0.0
        for y in range(3):
            local = local + own_frame[:, 3 * y + x : 3 * y + x + 1] * away[y]
        norm = norm + local * local
        item = dot(local.astype(BF16), narrow).astype(BF16)
        first = width + x * out_cols
        mixed = mixed + dot(item, w_out[first : first + out_cols, :])
    item = dot(jnp.sqrt(norm + 1e-08).astype(BF16), narrow).astype(BF16)
    first = width + 3 * out_cols
    mixed = mixed + dot(item, w_out[first : first + out_cols, :])
    first = first + out_cols
    for h in range(heads):
        item = attp[pl.ds(h, rows, stride=HP), :].astype(BF16)
        mixed = mixed + dot(item, w_out[first + h * pair_dim : first + (h + 1) * pair_dim, :])

    center = mixed - jnp.mean(mixed, axis=1, keepdims=True)
    var = jnp.mean(center * center, axis=1, keepdims=True)
    snew = center * lax.rsqrt(var + 1e-05) * out_gain[...]
    single_out[...] = snew.astype(BF16)
    update = jnp.dot(snew, w_frame[...], precision=lax.Precision.HIGHEST, preferred_element_type=F32)
    table = jnp.concatenate([update, own_frame, jnp.zeros((rows, 110), F32)], axis=1).T
    b, c, d = table[0:1], table[1:2], table[2:3]
    size = jnp.sqrt(1.0 + b * b + c * c + d * d)
    a = 1.0 / size
    b, c, d = b / size, c / size, d / size
    ru = [
        [a * a + b * b - c * c - d * d, 2.0 * (b * c - a * d), 2.0 * (b * d + a * c)],
        [2.0 * (b * c + a * d), a * a - b * b + c * c - d * d, 2.0 * (c * d - a * b)],
        [2.0 * (b * d - a * c), 2.0 * (c * d + a * b), a * a - b * b - c * c + d * d],
    ]
    rot = [[table[6 + 3 * x + y : 7 + 3 * x + y] for y in range(3)] for x in range(3)]
    for x in range(3):
        for z in range(3):
            frames_out[3 * x + z : 3 * x + z + 1, :] = (
                rot[x][0] * ru[0][z] + rot[x][1] * ru[1][z] + rot[x][2] * ru[2][z]
            )
        frames_out[9 + x : 10 + x, :] = (
            rot[x][0] * table[3:4] + rot[x][1] * table[4:5] + rot[x][2] * table[5:6]
            + table[15 + x : 16 + x]
        )

    @pl.loop(1, chips)
    def _(d):
        dev = peer_of(d)
        send(dev).wait_send()
        relay(dev).wait_send()

    send(sib).wait_send()


def exact_split(x):
    hi = lax.reduce_precision(x, 8, 7)
    mid = lax.reduce_precision(x - hi, 8, 7)
    return [hi, mid, x - hi - mid]


def per_device(
    n, single, angles, trans, left_factor, right_factor, chain, live, w_query, w_keyval, w_qpoints,
    w_kvpoints, w_pair_in, chain_bias, w_pair_out, w_bias, point_weight, w_out, out_gain, w_frame,
):
    rows, cs = single.shape
    heads = point_weight.shape[0]
    head_dim = w_query.shape[1] // heads
    qpts = w_qpoints.shape[1] // (3 * heads)
    vpts = w_kvpoints.shape[1] // (3 * heads) - qpts
    rank, pair_dim = w_pair_in.shape
    keys = n * rows
    frame = jnp.stack(rotation(angles) + [trans[0], trans[1], trans[2]]).T
    hot = (chain[:, None] == jnp.arange(CHAINS)[None, :]).astype(BF16)
    pad = AUX - rank - 3 * CHAINS - 37
    payload = jnp.concatenate(
        [single, right_factor, hot, hot, hot]
        + [item.astype(BF16) for item in exact_split(frame)]
        + [live.astype(BF16)[:, None], jnp.zeros((rows, pad), BF16)],
        axis=1,
    )
    left = jnp.concatenate(
        [left_factor, hot, hot, hot, jnp.zeros((rows, pad + 37), BF16)], axis=1
    ).astype(F32)
    coef = jnp.pad(point_weight * (2.0 / (9.0 * qpts)) ** 0.5 / 2.0, (0, HP - heads))[:, None]
    vmem = pl.BlockSpec(memory_space=pltpu.VMEM)
    hbm = pl.BlockSpec(memory_space=pl.ANY)
    pw = heads * (qpts + vpts)
    return pl.pallas_call(
        functools.partial(kernel, n, (heads, head_dim, qpts, vpts, rank, pair_dim)),
        out_shape=(
            jax.ShapeDtypeStruct((rows, cs), BF16),
            jax.ShapeDtypeStruct((12, rows), F32),
        ),
        in_specs=[vmem] * 9 + [hbm] * 5,
        out_specs=(vmem, vmem),
        scratch_shapes=[
            pltpu.VMEM((keys, cs + AUX), BF16),
            pltpu.VMEM(w_query.shape, BF16),
            pltpu.VMEM(w_keyval.shape, BF16),
            pltpu.VMEM(w_qpoints.shape, BF16),
            pltpu.VMEM(w_kvpoints.shape, BF16),
            pltpu.VMEM(w_out.shape, BF16),
            pltpu.VMEM((keys, w_keyval.shape[1]), BF16),
            pltpu.VMEM((3, keys, pw), BF16),
            pltpu.VMEM((rows * HP, keys), F32),
            pltpu.VMEM((rows * HP, keys), BF16),
            pltpu.VMEM((keys, 2 * pair_dim), BF16),
            pltpu.VMEM((rows * HP, pair_dim), F32),
            pltpu.VMEM((rows * HP, 128), F32),
            pltpu.VMEM((2 * AUX, 2 * pair_dim), BF16),
            pltpu.VMEM((2 * pair_dim, 2 * pair_dim), BF16),
            pltpu.VMEM((HP, keys), F32),
            pltpu.SemaphoreType.DMA((n,)),
            pltpu.SemaphoreType.DMA((n,)),
            pltpu.SemaphoreType.DMA((n,)),
            pltpu.SemaphoreType.DMA,
            pltpu.SemaphoreType.DMA((5,)),
        ],
        compiler_params=pltpu.CompilerParams(
            collective_id=0, has_side_effects=True, vmem_limit_bytes=50 * 1024 * 1024
        ),
    )(
        payload, left, coef, w_pair_in, chain_bias[None, :], w_pair_out, w_bias, out_gain[None, :],
        w_frame, w_query, w_keyval, w_qpoints, w_kvpoints, w_out,
    )


def solution(mesh):
    row = P("blk", None)
    col = P(None, "blk")
    in_specs = (row, col, col, row, row, P("blk"), P("blk")) + (P(),) * 12
    return jax.shard_map(
        functools.partial(per_device, mesh.shape["blk"]),
        mesh=mesh, in_specs=in_specs, out_specs=(row, col), check_vma=False,
    )
```

```python
import functools

import jax
import jax.numpy as jnp
from jax import lax
from jax.experimental import pallas as pl
from jax.experimental.pallas import tpu as pltpu
from jax.sharding import PartitionSpec as P

F32 = jnp.float32
BF16 = jnp.bfloat16
MESH = pl.DeviceIdType.MESH
HP = 16
CHAINS = 8
AUX = 128


def dot(a, b):
    return jnp.dot(a, b, preferred_element_type=F32)


def dot_t(a, b):
    return lax.dot_general(a, b, (((1,), (1,)), ((), ())), preferred_element_type=F32)


def split3(x):
    hi = x.astype(BF16)
    rest = x - hi.astype(F32)
    mid = rest.astype(BF16)
    lo = (rest - mid.astype(F32)).astype(BF16)
    return hi, mid, lo


def onehot(mask):
    return jnp.where(mask, 1.0, 0.0).astype(BF16)


def iota(shape, dim):
    return lax.broadcasted_iota(jnp.int32, shape, dim)


def frame_columns(aux, base):
    wide = aux.astype(F32)
    return (
        wide[:, base : base + 12] + wide[:, base + 12 : base + 24] + wide[:, base + 24 : base + 36]
    )


def flip(index, other, size):
    if size & (size - 1):
        return (index + other) % size
    out = 0
    bit = 1
    while bit < size:
        out = out + ((index // bit + other // bit) % 2) * bit
        bit *= 2
    return out


def kernel(
    n, dims, single, angles, trans, left_factor, right_factor, chain, live, coef_in,
    w_pair_in, chain_bias, w_pair_out, w_bias, out_gain, w_frame, w_query, w_qpoints,
    w_keyval_h, w_kvpoints_h, w_out_h,
    single_out, frames_out,
    payload, left, gat, w_keyval, w_kvpoints, w_out, wk2, kv, kgk, kgv, ksq, wts, pair, attp, scale,
    win2, wout2, dead,
    send_sem, recv_sem, relay_sem, own_sem, w_sem, logit,
):
    heads, head_dim, qpts, vpts, rank, pair_dim = dims
    rows, cs = single_out.shape
    keys = n * rows
    width = heads * head_dim
    pts = qpts + vpts
    pw = heads * pts
    part = heads * qpts
    out_cols = heads * vpts
    fbase = rank + 3 * CHAINS
    third = (1.0 / 3.0) ** 0.5
    me = lax.axis_index("blk")
    chips = n // 2
    core = me % 2
    chip = me // 2
    sib = chip * 2 + 1 - core
    kb = 128
    group = kb // (2 * rows)
    blocks = keys // kb

    loads = [
        pltpu.make_async_copy(src, dst, w_sem.at[i])
        for i, (src, dst) in enumerate(
            [(w_keyval_h, w_keyval), (w_kvpoints_h, w_kvpoints), (w_out_h, w_out)]
        )
    ]
    barrier = pltpu.get_barrier_semaphore()

    def peer_of(d):
        return flip(chip, d, chips) * 2 + core

    def block(dev):
        return gat.at[pl.ds(pl.multiple_of(dev * rows, rows), rows), :]

    @pl.loop(1, chips)
    def _(d):
        pl.semaphore_signal(barrier, inc=1, device_id=(peer_of(d),), device_id_type=MESH)

    pl.semaphore_signal(barrier, inc=1, device_id=(sib,), device_id_type=MESH)
    for item in loads:
        item.start()

    cos, sin = jnp.cos(angles[...]), jnp.sin(angles[...])
    ca, cb, cc = cos[0:1], cos[1:2], cos[2:3]
    sa, sb, sc = sin[0:1], sin[1:2], sin[2:3]
    frame_rows = [
        ca * cb, -sa * cc + ca * sb * sc, sa * sc + ca * sb * cc,
        sa * cb, ca * cc + sa * sb * sc, -ca * sc + sa * sb * cc,
        -sb, cb * sc, cb * cc,
        trans[0:1, :], trans[1:2, :], trans[2:3, :],
    ]
    chain_row = chain[...].reshape(1, rows)
    live_row = live[...].reshape(1, rows).astype(F32)
    hot = jnp.where(iota((3 * CHAINS, rows), 0) % CHAINS == chain_row, 1.0, 0.0)
    frames = jnp.concatenate(frame_rows, axis=0)
    table = jnp.concatenate(
        [hot]
        + [item.astype(F32) for item in split3(frames)]
        + [live_row, jnp.zeros((AUX - fbase - 37, rows), F32)],
        axis=0,
    )
    side = AUX - rank
    table = jnp.concatenate([table, jnp.zeros((side, 128 - rows), F32)], axis=1).T[:rows]
    payload[:, :cs] = single[...]
    payload[:, cs:] = jnp.concatenate([right_factor[...].astype(F32), table], axis=1).astype(BF16)
    left[...] = jnp.concatenate(
        [left_factor[...].astype(F32), jnp.where(iota(table.shape, 1) < 3 * CHAINS, table, 0.0)],
        axis=1,
    )
    pl.semaphore_wait(barrier, chips)
    own = pltpu.make_async_copy(payload, block(me), own_sem)
    own.start()

    def send(dev):
        return pltpu.make_async_remote_copy(
            src_ref=payload, dst_ref=block(me), send_sem=send_sem.at[dev], recv_sem=recv_sem.at[me],
            device_id=(dev,), device_id_type=MESH,
        )

    def arrival(dev):
        return pltpu.make_async_remote_copy(
            src_ref=payload, dst_ref=block(dev), send_sem=send_sem.at[dev],
            recv_sem=recv_sem.at[dev], device_id=(sib,), device_id_type=MESH,
        )

    def relay(dev):
        return pltpu.make_async_remote_copy(
            src_ref=block(dev), dst_ref=block(dev), send_sem=relay_sem.at[dev],
            recv_sem=recv_sem.at[dev], device_id=(sib,), device_id_type=MESH,
        )

    send(sib).start()

    @pl.loop(1, chips)
    def _(d):
        send(peer_of(d)).start()

    own_x = single[...]
    own_frame = frame_columns(payload[:, cs:], fbase)
    query = dot_t(own_x, w_query[...]).astype(BF16).astype(F32)
    hrow = iota((rows, HP, width), 1)
    lane = iota((rows, HP, width), 2)
    vmask = ((lane >= hrow * head_dim) & (lane < (hrow + 1) * head_dim)).reshape(rows * HP, width)
    a_query = jnp.where(
        vmask, jnp.broadcast_to(query[:, None, :], (rows, HP, width)).reshape(rows * HP, width), 0.0
    ).astype(BF16)
    place = iota((128, part), 0)
    twice = onehot(
        (place == iota((128, part), 1)) | (place == iota((128, part), 1) + part)
    )
    qp = [
        dot_t(own_x, dot(twice, w_qpoints[y * part : (y + 1) * part, :]).astype(BF16))
        for y in range(3)
    ]
    hrow = iota((rows, HP, 128), 1)
    lane = iota((rows, HP, 128), 2)
    mask_hi = ((lane >= hrow * qpts) & (lane < (hrow + 1) * qpts)).reshape(rows * HP, 128)
    mask_mid = (
        (lane >= part + hrow * qpts) & (lane < part + (hrow + 1) * qpts)
    ).reshape(rows * HP, 128)
    amask = ((lane >= hrow * vpts) & (lane < (hrow + 1) * vpts)).reshape(rows * HP, 128)
    a_first, a_last = [], []
    qsum = 0.0
    for x in range(3):
        point = own_frame[:, 9 + x : 10 + x]
        for y in range(3):
            point = point + own_frame[:, 3 * x + y : 3 * x + y + 1] * qp[y]
        point = jnp.broadcast_to(point[:, None, :], (rows, HP, 128)).reshape(rows * HP, 128)
        only = jnp.where(mask_hi, point, 0.0)
        qsum = qsum + only * only
        hi, mid, lo = [item.astype(F32) for item in split3(point)]
        a_first.append(jnp.where(mask_hi, hi, jnp.where(mask_mid, mid, 0.0)).astype(BF16))
        a_last.append(jnp.where(mask_hi, lo, 0.0).astype(BF16))
    a_first = jnp.concatenate(a_first, axis=1)
    a_last = jnp.concatenate(a_last, axis=1)
    qsq = jnp.sum(qsum, axis=1, keepdims=True)
    diag = iota((HP, heads), 0) == iota((HP, heads), 1)
    factor = (2.0 / (9.0 * qpts)) ** 0.5 / 2.0
    coef16 = jnp.sum(
        jnp.where(diag, coef_in[...].reshape(1, heads) * factor, 0.0), axis=1, keepdims=True
    )
    coef = jnp.broadcast_to(coef16[None], (rows, HP, 1)).reshape(rows * HP, 1)

    def twin(block_w):
        none = jnp.zeros(block_w.shape, block_w.dtype)
        return jnp.concatenate(
            [
                jnp.concatenate([block_w, none], axis=1),
                jnp.concatenate([none, block_w], axis=1),
            ],
            axis=0,
        )

    bias_parts = [
        jnp.broadcast_to(item.astype(F32), (CHAINS, pair_dim))
        for item in split3(chain_bias[...].reshape(1, pair_dim))
    ]
    win2[...] = twin(
        jnp.concatenate(
            [w_pair_in[...].astype(F32)] + bias_parts + [jnp.zeros((AUX - fbase, pair_dim), F32)],
            axis=0,
        ).astype(BF16)
    )
    w_o = w_pair_out[...].astype(F32)
    w_o = w_o - jnp.mean(w_o, axis=1, keepdims=True)
    w_hi = w_o.astype(BF16)
    wout2[0] = twin(w_hi)
    wout2[1] = twin((w_o - w_hi.astype(F32)).astype(BF16))
    wout2[2] = twin(jnp.full((pair_dim, pair_dim), 1.0 / pair_dim, BF16))
    w_b2 = twin(dot(onehot(diag), w_bias[...]).astype(BF16))

    loads[0].wait()
    loads[1].wait()
    place = iota((256, pw), 0)
    source = iota((256, pw), 1)
    kcol = (source // pts) * qpts + source % pts
    vcol = 128 + (source // pts) * vpts + source % pts - qpts
    is_key = source % pts < qpts
    order = onehot(
        (is_key & ((place == kcol) | (place == kcol + part))) | ((source % pts >= qpts) & (place == vcol))
    )
    for y in range(3):
        wk2[y * 256 : (y + 1) * 256, :] = dot(
            order, w_kvpoints[y * pw : (y + 1) * pw, :]
        ).astype(BF16)

    hrow = iota((HP, 128), 0)
    lane = iota((HP, 128), 1)
    hsel = onehot((lane >= hrow * qpts) & (lane < (hrow + 1) * qpts))
    live_sel = onehot(iota((HP, AUX), 1) == fbase + 36)

    def forward(k, first):
        @pl.loop(first, group)
        def _(j):
            dev = peer_of(k * group + j)
            arrival(dev).wait_recv()
            relay(dev).start()

    def settle(k, first):
        @pl.loop(first, group)
        def _(j):
            arrival(flip(chip, k * group + j, chips) * 2 + 1 - core).wait_recv()

    forward(0, 1)
    own.wait()
    arrival(sib).wait_recv()
    settle(0, 1)

    @pl.loop(0, blocks)
    def _(k):
        base = flip(chip // group, k, blocks) * kb
        at = pl.ds(pl.multiple_of(base, kb), kb)
        x_in = gat[at, :cs]
        aux = gat[at, cs:]
        kv[at, :] = dot(x_in, w_keyval[...]).astype(BF16)
        kp = dot_t(x_in, wk2[...])
        frame = frame_columns(aux, fbase)
        square = 0.0
        for x in range(3):
            point = frame[:, 9 + x : 10 + x]
            for y in range(3):
                point = point + frame[:, 3 * x + y : 3 * x + y + 1] * kp[:, y * 256 : (y + 1) * 256]
            point = point.astype(BF16)
            kgk[at, x * 128 : (x + 1) * 128] = point[:, :128]
            kgv[at, x * 128 : (x + 1) * 128] = point[:, 128:]
            wide = point[:, :128].astype(F32)
            square = square + wide * wide
        total = 0.0
        for item in split3(square):
            total = total + dot_t(hsel, item)
        ksq[:, at] = total
        dead[:, at] = 100000.0 * (1.0 - dot_t(live_sel, aux))

        @pl.when(k + 1 < blocks)
        def _():
            forward(k + 1, 0)

        @pl.loop(0, rows // 2, unroll=2)
        def _(t):
            right = aux.astype(F32)
            prod = jnp.concatenate(
                [
                    (right * left[pl.ds(2 * t, 1), :]).astype(BF16),
                    (right * left[pl.ds(2 * t + 1, 1), :]).astype(BF16),
                ],
                axis=1,
            )
            hidden = dot(prod, win2[...])
            hidden = jax.nn.gelu(hidden, approximate=True).astype(BF16)
            center = dot(hidden, wout2[0]) + dot(hidden, wout2[1])
            for half in range(2):
                o = center[:, half * pair_dim : (half + 1) * pair_dim]
                var = jnp.mean(o * o, axis=1, keepdims=True)
                pair[t, at, half * pair_dim : (half + 1) * pair_dim] = (
                    o * lax.rsqrt(var + 1e-05)
                ).astype(BF16)

        @pl.when(k + 1 < blocks)
        def _():
            settle(k + 1, 0)

    both_dead = jnp.concatenate([dead[...], dead[...]], axis=0)
    kstep = 512 if keys % 512 == 0 else kb

    @pl.loop(0, keys // kstep)
    def _(b):
        at = pl.ds(pl.multiple_of(b * kstep, kstep), kstep)
        near = kgk[at, :]
        cross = dot_t(a_first, near) + dot_t(a_last, near)
        scalar = dot_t(a_query, kv[at, :width]) * head_dim ** (-0.5)
        square = jnp.broadcast_to(ksq[:, at][None], (rows, HP, kstep)).reshape(rows * HP, kstep)
        logit[:, at] = scalar - coef * (qsq + square - 2.0 * cross)

    @pl.loop(0, rows // 2, unroll=2)
    def _(t):
        sel = pl.ds(pl.multiple_of(t * 2 * HP, 2 * HP), 2 * HP)
        both = pair[t]
        bias = dot_t(w_b2, both)
        row = third * (logit[sel, :] + bias) - both_dead
        top = jnp.max(row, axis=1, keepdims=True)
        terms = jnp.exp(row - top)
        inv = 1.0 / jnp.sum(terms, axis=1, keepdims=True)
        weight = terms.astype(BF16)
        wts[sel, :] = weight
        scale[sel, :] = jnp.broadcast_to(inv, (2 * HP, 128))
        out = dot(weight, both) * inv
        attp[sel, :] = jnp.concatenate([out[:HP, :pair_dim], out[HP:, pair_dim:]], axis=0)

    weight = wts[...]
    inv = scale[:, :1]

    def pick(value, mask):
        value = jnp.where(mask, value * inv, 0.0)
        return jnp.sum(value.reshape(rows, HP, value.shape[1]), axis=1)

    values = pick(dot(weight, kv[:, width:]), vmask)
    points = dot(weight, kgv[...])
    away = [
        pick(points[:, y * 128 : (y + 1) * 128], amask) - own_frame[:, 9 + y : 10 + y]
        for y in range(3)
    ]
    loads[2].wait()
    mixed = own_x.astype(F32) + dot(values.astype(BF16), w_out[:width, :])
    norm = 0.0
    for x in range(3):
        local = 0.0
        for y in range(3):
            local = local + own_frame[:, 3 * y + x : 3 * y + x + 1] * away[y]
        norm = norm + local * local
        first = width + x * out_cols
        mixed = mixed + dot(local[:, :out_cols].astype(BF16), w_out[first : first + out_cols, :])
    first = width + 3 * out_cols
    item = jnp.sqrt(norm + 1e-08)[:, :out_cols].astype(BF16)
    mixed = mixed + dot(item, w_out[first : first + out_cols, :])
    first = first + out_cols
    for h in range(heads):
        item = attp[pl.ds(h, rows, stride=HP), :].astype(BF16)
        mixed = mixed + dot(item, w_out[first + h * pair_dim : first + (h + 1) * pair_dim, :])

    center = mixed - jnp.mean(mixed, axis=1, keepdims=True)
    var = jnp.mean(center * center, axis=1, keepdims=True)
    snew = center * lax.rsqrt(var + 1e-05) * out_gain[...].reshape(1, cs)
    single_out[...] = snew.astype(BF16)
    update = lax.dot_general(
        w_frame[...], snew, (((1,), (1,)), ((), ())),
        precision=lax.Precision.HIGHEST, preferred_element_type=F32,
    )
    b, c, d = update[0:1], update[1:2], update[2:3]
    size = jnp.sqrt(1.0 + b * b + c * c + d * d)
    a = 1.0 / size
    b, c, d = b / size, c / size, d / size
    ru = [
        [a * a + b * b - c * c - d * d, 2.0 * (b * c - a * d), 2.0 * (b * d + a * c)],
        [2.0 * (b * c + a * d), a * a - b * b + c * c - d * d, 2.0 * (c * d - a * b)],
        [2.0 * (b * d - a * c), 2.0 * (c * d + a * b), a * a - b * b - c * c + d * d],
    ]
    for x in range(3):
        r0, r1, r2 = frame_rows[3 * x : 3 * x + 3]
        for z in range(3):
            frames_out[3 * x + z : 3 * x + z + 1, :] = r0 * ru[0][z] + r1 * ru[1][z] + r2 * ru[2][z]
        frames_out[9 + x : 10 + x, :] = (
            r0 * update[3:4] + r1 * update[4:5] + r2 * update[5:6] + frame_rows[9 + x]
        )

    @pl.loop(1, chips)
    def _(d):
        dev = peer_of(d)
        send(dev).wait_send()
        relay(dev).wait_send()

    send(sib).wait_send()


def per_device(
    n, single, angles, trans, left_factor, right_factor, chain, live, w_query, w_keyval, w_qpoints,
    w_kvpoints, w_pair_in, chain_bias, w_pair_out, w_bias, point_weight, w_out, out_gain, w_frame,
):
    rows, cs = single.shape
    heads = point_weight.shape[0]
    head_dim = w_query.shape[1] // heads
    qpts = w_qpoints.shape[1] // (3 * heads)
    vpts = w_kvpoints.shape[1] // (3 * heads) - qpts
    rank, pair_dim = w_pair_in.shape
    keys = n * rows
    vmem = pl.BlockSpec(memory_space=pltpu.VMEM)
    hbm = pl.BlockSpec(memory_space=pltpu.HBM)
    return pl.pallas_call(
        functools.partial(kernel, n, (heads, head_dim, qpts, vpts, rank, pair_dim)),
        out_shape=(
            jax.ShapeDtypeStruct((rows, cs), BF16),
            jax.ShapeDtypeStruct((12, rows), F32),
        ),
        in_specs=[vmem] * 16 + [hbm] * 3,
        out_specs=(vmem, vmem),
        scratch_shapes=[
            pltpu.VMEM((rows, cs + AUX), BF16),
            pltpu.VMEM((rows, AUX), F32),
            pltpu.VMEM((keys, cs + AUX), BF16),
            pltpu.VMEM(w_keyval.shape, BF16),
            pltpu.VMEM(w_kvpoints.shape[::-1], BF16),
            pltpu.VMEM(w_out.shape, BF16),
            pltpu.VMEM((3 * 256, cs), BF16),
            pltpu.VMEM((keys, w_keyval.shape[1]), BF16),
            pltpu.VMEM((keys, 3 * 128), BF16),
            pltpu.VMEM((keys, 3 * 128), BF16),
            pltpu.VMEM((HP, keys), F32),
            pltpu.VMEM((rows * HP, keys), BF16),
            pltpu.VMEM((rows // 2, keys, 2 * pair_dim), BF16),
            pltpu.VMEM((rows * HP, pair_dim), F32),
            pltpu.VMEM((rows * HP, 128), F32),
            pltpu.VMEM((2 * AUX, 2 * pair_dim), BF16),
            pltpu.VMEM((3, 2 * pair_dim, 2 * pair_dim), BF16),
            pltpu.VMEM((HP, keys), F32),
            pltpu.SemaphoreType.DMA((n,)),
            pltpu.SemaphoreType.DMA((n,)),
            pltpu.SemaphoreType.DMA((n,)),
            pltpu.SemaphoreType.DMA,
            pltpu.SemaphoreType.DMA((3,)),
            pltpu.VMEM((rows * HP, keys), F32),
        ],
        compiler_params=pltpu.CompilerParams(
            collective_id=0, has_side_effects=True, vmem_limit_bytes=50 * 1024 * 1024
        ),
    )(
        single, angles, trans, left_factor, right_factor, chain, live, point_weight,
        w_pair_in, chain_bias, w_pair_out, w_bias.T, out_gain, w_frame.T, w_query.T, w_qpoints.T,
        w_keyval, w_kvpoints.T, w_out,
    )


def solution(mesh):
    row = P("blk", None)
    col = P(None, "blk")
    in_specs = (row, col, col, row, row, P("blk"), P("blk")) + (P(),) * 12
    return jax.shard_map(
        functools.partial(per_device, mesh.shape["blk"]),
        mesh=mesh, in_specs=in_specs, out_specs=(row, col), check_vma=False,
    )
```

```python
import functools

import jax
import jax.numpy as jnp
from jax import lax
from jax.experimental import pallas as pl
from jax.experimental.pallas import tpu as pltpu
from jax.sharding import PartitionSpec as P

F32 = jnp.float32
BF16 = jnp.bfloat16
MESH = pl.DeviceIdType.MESH
HP = 16
CHAINS = 8
AUX = 128


def dot(a, b):
    return jnp.dot(a, b, preferred_element_type=F32)


def dot_t(a, b):
    return lax.dot_general(a, b, (((1,), (1,)), ((), ())), preferred_element_type=F32)


def split3(x):
    hi = x.astype(BF16)
    rest = x - hi.astype(F32)
    mid = rest.astype(BF16)
    lo = (rest - mid.astype(F32)).astype(BF16)
    return hi, mid, lo


def onehot(mask):
    return jnp.where(mask, 1.0, 0.0).astype(BF16)


def iota(shape, dim):
    return lax.broadcasted_iota(jnp.int32, shape, dim)


def frame_columns(aux, base):
    wide = aux.astype(F32)
    return (
        wide[:, base : base + 12] + wide[:, base + 12 : base + 24] + wide[:, base + 24 : base + 36]
    )


def flip(index, other, size):
    if size & (size - 1):
        return (index + other) % size
    out = 0
    bit = 1
    while bit < size:
        out = out + ((index // bit + other // bit) % 2) * bit
        bit *= 2
    return out


def kernel(
    n, dims, *refs,
):
    sources = refs[:19]
    single_out, frames_out = refs[19:21]
    held = refs[21:40]
    (
        payload, left, gat, wk2, kv, kgk, kgv, ksq, wts, pair, attp, scale, win2, wout2, dead,
        send_sem, recv_sem, relay_sem, own_sem, w_sem, logit, bias_rows,
    ) = refs[40:]
    (
        single, angles, trans, left_factor, right_factor, chain, live, coef_in, w_pair_in,
        chain_bias, w_pair_out, w_bias, out_gain, w_frame, w_query, w_qpoints, w_keyval,
        w_kvpoints, w_out,
    ) = held
    heads, head_dim, qpts, vpts, rank, pair_dim = dims
    rows, cs = single_out.shape
    keys = n * rows
    width = heads * head_dim
    pts = qpts + vpts
    pw = heads * pts
    part = heads * qpts
    out_cols = heads * vpts
    fbase = rank + 3 * CHAINS
    third = (1.0 / 3.0) ** 0.5
    me = lax.axis_index("blk")
    chips = n // 2
    core = me % 2
    chip = me // 2
    sib = chip * 2 + 1 - core
    kb = 128
    group = kb // (2 * rows)
    blocks = keys // kb

    loads = [
        pltpu.make_async_copy(src, dst, w_sem.at[i])
        for i, (src, dst) in enumerate(zip(sources, held))
    ]
    for item in loads:
        item.start()
    barrier = pltpu.get_barrier_semaphore()

    def peer_of(d):
        return flip(chip, d, chips) * 2 + core

    def block(dev):
        return gat.at[pl.ds(pl.multiple_of(dev * rows, rows), rows), :]

    @pl.loop(1, chips)
    def _(d):
        pl.semaphore_signal(barrier, inc=1, device_id=(peer_of(d),), device_id_type=MESH)

    pl.semaphore_signal(barrier, inc=1, device_id=(sib,), device_id_type=MESH)
    for item in loads[:7]:
        item.wait()

    cos, sin = jnp.cos(angles[...]), jnp.sin(angles[...])
    ca, cb, cc = cos[0:1], cos[1:2], cos[2:3]
    sa, sb, sc = sin[0:1], sin[1:2], sin[2:3]
    frame_rows = [
        ca * cb, -sa * cc + ca * sb * sc, sa * sc + ca * sb * cc,
        sa * cb, ca * cc + sa * sb * sc, -ca * sc + sa * sb * cc,
        -sb, cb * sc, cb * cc,
        trans[0:1, :], trans[1:2, :], trans[2:3, :],
    ]
    chain_row = chain[...].reshape(1, rows)
    live_row = live[...].reshape(1, rows).astype(F32)
    hot = jnp.where(iota((3 * CHAINS, rows), 0) % CHAINS == chain_row, 1.0, 0.0)
    frames = jnp.concatenate(frame_rows, axis=0)
    table = jnp.concatenate(
        [hot]
        + [item.astype(F32) for item in split3(frames)]
        + [live_row, jnp.zeros((AUX - fbase - 37, rows), F32)],
        axis=0,
    )
    side = AUX - rank
    table = jnp.concatenate([table, jnp.zeros((side, 128 - rows), F32)], axis=1).T[:rows]
    payload[:, :cs] = single[...]
    payload[:, cs:] = jnp.concatenate([right_factor[...].astype(F32), table], axis=1).astype(BF16)
    left[...] = jnp.concatenate(
        [left_factor[...].astype(F32), jnp.where(iota(table.shape, 1) < 3 * CHAINS, table, 0.0)],
        axis=1,
    )
    pl.semaphore_wait(barrier, chips)
    own = pltpu.make_async_copy(payload, block(me), own_sem)
    own.start()

    def send(dev):
        return pltpu.make_async_remote_copy(
            src_ref=payload, dst_ref=block(me), send_sem=send_sem.at[dev], recv_sem=recv_sem.at[me],
            device_id=(dev,), device_id_type=MESH,
        )

    def arrival(dev):
        return pltpu.make_async_remote_copy(
            src_ref=payload, dst_ref=block(dev), send_sem=send_sem.at[dev],
            recv_sem=recv_sem.at[dev], device_id=(sib,), device_id_type=MESH,
        )

    def relay(dev):
        return pltpu.make_async_remote_copy(
            src_ref=block(dev), dst_ref=block(dev), send_sem=relay_sem.at[dev],
            recv_sem=recv_sem.at[dev], device_id=(sib,), device_id_type=MESH,
        )

    send(sib).start()

    @pl.loop(1, chips)
    def _(d):
        send(peer_of(d)).start()

    for item in loads[7:16]:
        item.wait()
    own_x = single[...]
    own_frame = frame_columns(payload[:, cs:], fbase)
    query = dot_t(own_x, w_query[...]).astype(BF16).astype(F32)
    hrow = iota((rows, HP, width), 1)
    lane = iota((rows, HP, width), 2)
    vmask = ((lane >= hrow * head_dim) & (lane < (hrow + 1) * head_dim)).reshape(rows * HP, width)
    a_query = jnp.where(
        vmask, jnp.broadcast_to(query[:, None, :], (rows, HP, width)).reshape(rows * HP, width), 0.0
    ).astype(BF16)
    place = iota((128, part), 0)
    twice = onehot(
        (place == iota((128, part), 1)) | (place == iota((128, part), 1) + part)
    )
    qp = [
        dot_t(own_x, dot(twice, w_qpoints[y * part : (y + 1) * part, :]).astype(BF16))
        for y in range(3)
    ]
    hrow = iota((rows, HP, 128), 1)
    lane = iota((rows, HP, 128), 2)
    mask_hi = ((lane >= hrow * qpts) & (lane < (hrow + 1) * qpts)).reshape(rows * HP, 128)
    mask_mid = (
        (lane >= part + hrow * qpts) & (lane < part + (hrow + 1) * qpts)
    ).reshape(rows * HP, 128)
    amask = ((lane >= hrow * vpts) & (lane < (hrow + 1) * vpts)).reshape(rows * HP, 128)
    a_first, a_last = [], []
    qsum = 0.0
    for x in range(3):
        point = own_frame[:, 9 + x : 10 + x]
        for y in range(3):
            point = point + own_frame[:, 3 * x + y : 3 * x + y + 1] * qp[y]
        point = jnp.broadcast_to(point[:, None, :], (rows, HP, 128)).reshape(rows * HP, 128)
        only = jnp.where(mask_hi, point, 0.0)
        qsum = qsum + only * only
        hi, mid, lo = [item.astype(F32) for item in split3(point)]
        a_first.append(jnp.where(mask_hi, hi, jnp.where(mask_mid, mid, 0.0)).astype(BF16))
        a_last.append(jnp.where(mask_hi, lo, 0.0).astype(BF16))
    a_first = jnp.concatenate(a_first, axis=1)
    a_last = jnp.concatenate(a_last, axis=1)
    qsq = jnp.sum(qsum, axis=1, keepdims=True)
    diag = iota((HP, heads), 0) == iota((HP, heads), 1)
    factor = (2.0 / (9.0 * qpts)) ** 0.5 / 2.0
    coef16 = jnp.sum(
        jnp.where(diag, coef_in[...].reshape(1, heads) * factor, 0.0), axis=1, keepdims=True
    )
    coef = jnp.broadcast_to(coef16[None], (rows, HP, 1)).reshape(rows * HP, 1)

    def twin(block_w):
        none = jnp.zeros(block_w.shape, block_w.dtype)
        return jnp.concatenate(
            [
                jnp.concatenate([block_w, none], axis=1),
                jnp.concatenate([none, block_w], axis=1),
            ],
            axis=0,
        )

    bias_parts = [
        jnp.broadcast_to(item.astype(F32), (CHAINS, pair_dim))
        for item in split3(chain_bias[...].reshape(1, pair_dim))
    ]
    win2[...] = twin(
        jnp.concatenate(
            [w_pair_in[...].astype(F32)] + bias_parts + [jnp.zeros((AUX - fbase, pair_dim), F32)],
            axis=0,
        ).astype(BF16)
    )
    w_o = w_pair_out[...].astype(F32)
    w_o = w_o - jnp.mean(w_o, axis=1, keepdims=True)
    w_hi = w_o.astype(BF16)
    wout2[0] = twin(w_hi)
    wout2[1] = twin((w_o - w_hi.astype(F32)).astype(BF16))
    wout2[2] = twin(jnp.full((pair_dim, pair_dim), 1.0 / pair_dim, BF16))
    w_b2 = twin(dot(onehot(diag), w_bias[...]).astype(BF16))

    loads[16].wait()
    loads[17].wait()
    place = iota((256, pw), 0)
    source = iota((256, pw), 1)
    kcol = (source // pts) * qpts + source % pts
    vcol = 128 + (source // pts) * vpts + source % pts - qpts
    is_key = source % pts < qpts
    order = onehot(
        (is_key & ((place == kcol) | (place == kcol + part))) | ((source % pts >= qpts) & (place == vcol))
    )
    for y in range(3):
        wk2[y * 256 : (y + 1) * 256, :] = dot(
            order, w_kvpoints[y * pw : (y + 1) * pw, :]
        ).astype(BF16)

    hrow = iota((HP, 128), 0)
    lane = iota((HP, 128), 1)
    hsel = onehot((lane >= hrow * qpts) & (lane < (hrow + 1) * qpts))
    live_sel = onehot(iota((HP, AUX), 1) == fbase + 36)

    def forward(k, first):
        @pl.loop(first, group)
        def _(j):
            dev = peer_of(k * group + j)
            arrival(dev).wait_recv()
            relay(dev).start()

    def settle(k, first):
        @pl.loop(first, group)
        def _(j):
            arrival(flip(chip, k * group + j, chips) * 2 + 1 - core).wait_recv()

    forward(0, 1)
    own.wait()
    arrival(sib).wait_recv()
    settle(0, 1)

    @pl.loop(0, blocks)
    def _(k):
        base = flip(chip // group, k, blocks) * kb
        at = pl.ds(pl.multiple_of(base, kb), kb)
        x_in = gat[at, :cs]
        aux = gat[at, cs:]
        kv[at, :] = dot(x_in, w_keyval[...]).astype(BF16)
        kp = dot_t(x_in, wk2[...])
        frame = frame_columns(aux, fbase)
        square = 0.0
        for x in range(3):
            point = frame[:, 9 + x : 10 + x]
            for y in range(3):
                point = point + frame[:, 3 * x + y : 3 * x + y + 1] * kp[:, y * 256 : (y + 1) * 256]
            point = point.astype(BF16)
            kgk[at, x * 128 : (x + 1) * 128] = point[:, :128]
            kgv[at, x * 128 : (x + 1) * 128] = point[:, 128:]
            wide = point[:, :128].astype(F32)
            square = square + wide * wide
        total = 0.0
        for item in split3(square):
            total = total + dot_t(hsel, item)
        ksq[:, at] = total
        dead[:, at] = 100000.0 * (1.0 - dot_t(live_sel, aux))

        @pl.when(k + 1 < blocks)
        def _():
            forward(k + 1, 0)

        @pl.loop(0, rows // 2, unroll=2)
        def _(t):
            right = aux.astype(F32)
            prod = jnp.concatenate(
                [
                    (right * left[pl.ds(2 * t, 1), :]).astype(BF16),
                    (right * left[pl.ds(2 * t + 1, 1), :]).astype(BF16),
                ],
                axis=1,
            )
            hidden = dot(prod, win2[...])
            hidden = jax.nn.gelu(hidden, approximate=True).astype(BF16)
            center = dot(hidden, wout2[0]) + dot(hidden, wout2[1])
            normed = []
            for half in range(2):
                o = center[:, half * pair_dim : (half + 1) * pair_dim]
                var = jnp.mean(o * o, axis=1, keepdims=True)
                normed.append((o * lax.rsqrt(var + 1e-05)).astype(BF16))
            normed = jnp.concatenate(normed, axis=1)
            pair[t, at, :] = normed
            sel = pl.ds(pl.multiple_of(t * 2 * HP, 2 * HP), 2 * HP)
            bias_rows[sel, at] = dot_t(w_b2, normed)

        @pl.when(k + 1 < blocks)
        def _():
            settle(k + 1, 0)

    both_dead = jnp.concatenate([dead[...], dead[...]], axis=0)
    kstep = 512 if keys % 512 == 0 else kb

    @pl.loop(0, keys // kstep)
    def _(b):
        at = pl.ds(pl.multiple_of(b * kstep, kstep), kstep)
        near = kgk[at, :]
        cross = dot_t(a_first, near) + dot_t(a_last, near)
        scalar = dot_t(a_query, kv[at, :width]) * head_dim ** (-0.5)
        square = jnp.broadcast_to(ksq[:, at][None], (rows, HP, kstep)).reshape(rows * HP, kstep)
        logit[:, at] = scalar - coef * (qsq + square - 2.0 * cross)

    @pl.loop(0, rows // 2, unroll=4)
    def _(t):
        sel = pl.ds(pl.multiple_of(t * 2 * HP, 2 * HP), 2 * HP)
        both = pair[t]
        row = third * (logit[sel, :] + bias_rows[sel, :]) - both_dead
        top = jnp.max(row, axis=1, keepdims=True)
        terms = jnp.exp(row - top)
        inv = 1.0 / jnp.sum(terms, axis=1, keepdims=True)
        weight = terms.astype(BF16)
        wts[sel, :] = weight
        scale[sel, :] = jnp.broadcast_to(inv, (2 * HP, 128))
        out = dot(weight, both) * inv
        attp[sel, :] = jnp.concatenate([out[:HP, :pair_dim], out[HP:, pair_dim:]], axis=0)

    weight = wts[...]
    inv = scale[:, :1]

    def pick(value, mask):
        value = jnp.where(mask, value * inv, 0.0)
        return jnp.sum(value.reshape(rows, HP, value.shape[1]), axis=1)

    values = pick(dot(weight, kv[:, width:]), vmask)
    points = dot(weight, kgv[...])
    away = [
        pick(points[:, y * 128 : (y + 1) * 128], amask) - own_frame[:, 9 + y : 10 + y]
        for y in range(3)
    ]
    loads[18].wait()
    mixed = own_x.astype(F32) + dot(values.astype(BF16), w_out[:width, :])
    norm = 0.0
    for x in range(3):
        local = 0.0
        for y in range(3):
            local = local + own_frame[:, 3 * y + x : 3 * y + x + 1] * away[y]
        norm = norm + local * local
        first = width + x * out_cols
        mixed = mixed + dot(local[:, :out_cols].astype(BF16), w_out[first : first + out_cols, :])
    first = width + 3 * out_cols
    item = jnp.sqrt(norm + 1e-08)[:, :out_cols].astype(BF16)
    mixed = mixed + dot(item, w_out[first : first + out_cols, :])
    first = first + out_cols
    for h in range(heads):
        item = attp[pl.ds(h, rows, stride=HP), :].astype(BF16)
        mixed = mixed + dot(item, w_out[first + h * pair_dim : first + (h + 1) * pair_dim, :])

    center = mixed - jnp.mean(mixed, axis=1, keepdims=True)
    var = jnp.mean(center * center, axis=1, keepdims=True)
    snew = center * lax.rsqrt(var + 1e-05) * out_gain[...].reshape(1, cs)
    single_out[...] = snew.astype(BF16)
    update = lax.dot_general(
        w_frame[...], snew, (((1,), (1,)), ((), ())),
        precision=lax.Precision.HIGHEST, preferred_element_type=F32,
    )
    b, c, d = update[0:1], update[1:2], update[2:3]
    size = jnp.sqrt(1.0 + b * b + c * c + d * d)
    a = 1.0 / size
    b, c, d = b / size, c / size, d / size
    ru = [
        [a * a + b * b - c * c - d * d, 2.0 * (b * c - a * d), 2.0 * (b * d + a * c)],
        [2.0 * (b * c + a * d), a * a - b * b + c * c - d * d, 2.0 * (c * d - a * b)],
        [2.0 * (b * d - a * c), 2.0 * (c * d + a * b), a * a - b * b - c * c + d * d],
    ]
    for x in range(3):
        r0, r1, r2 = frame_rows[3 * x : 3 * x + 3]
        for z in range(3):
            frames_out[3 * x + z : 3 * x + z + 1, :] = r0 * ru[0][z] + r1 * ru[1][z] + r2 * ru[2][z]
        frames_out[9 + x : 10 + x, :] = (
            r0 * update[3:4] + r1 * update[4:5] + r2 * update[5:6] + frame_rows[9 + x]
        )

    @pl.loop(1, chips)
    def _(d):
        dev = peer_of(d)
        send(dev).wait_send()
        relay(dev).wait_send()

    send(sib).wait_send()


def per_device(
    n, single, angles, trans, left_factor, right_factor, chain, live, w_query, w_keyval, w_qpoints,
    w_kvpoints, w_pair_in, chain_bias, w_pair_out, w_bias, point_weight, w_out, out_gain, w_frame,
):
    rows, cs = single.shape
    heads = point_weight.shape[0]
    head_dim = w_query.shape[1] // heads
    qpts = w_qpoints.shape[1] // (3 * heads)
    vpts = w_kvpoints.shape[1] // (3 * heads) - qpts
    rank, pair_dim = w_pair_in.shape
    keys = n * rows
    vmem = pl.BlockSpec(memory_space=pltpu.VMEM)
    hbm = pl.BlockSpec(memory_space=pltpu.HBM)
    args = (
        single, angles, trans, left_factor, right_factor, chain, live, point_weight,
        w_pair_in, chain_bias, w_pair_out, w_bias.T, out_gain, w_frame.T, w_query.T, w_qpoints.T,
        w_keyval, w_kvpoints.T, w_out,
    )
    return pl.pallas_call(
        functools.partial(kernel, n, (heads, head_dim, qpts, vpts, rank, pair_dim)),
        out_shape=(
            jax.ShapeDtypeStruct((rows, cs), BF16),
            jax.ShapeDtypeStruct((12, rows), F32),
        ),
        in_specs=[hbm] * len(args),
        out_specs=(vmem, vmem),
        scratch_shapes=[pltpu.VMEM(item.shape, item.dtype) for item in args] + [
            pltpu.VMEM((rows, cs + AUX), BF16),
            pltpu.VMEM((rows, AUX), F32),
            pltpu.VMEM((keys, cs + AUX), BF16),
            pltpu.VMEM((3 * 256, cs), BF16),
            pltpu.VMEM((keys, w_keyval.shape[1]), BF16),
            pltpu.VMEM((keys, 3 * 128), BF16),
            pltpu.VMEM((keys, 3 * 128), BF16),
            pltpu.VMEM((HP, keys), F32),
            pltpu.VMEM((rows * HP, keys), BF16),
            pltpu.VMEM((rows // 2, keys, 2 * pair_dim), BF16),
            pltpu.VMEM((rows * HP, pair_dim), F32),
            pltpu.VMEM((rows * HP, 128), F32),
            pltpu.VMEM((2 * AUX, 2 * pair_dim), BF16),
            pltpu.VMEM((3, 2 * pair_dim, 2 * pair_dim), BF16),
            pltpu.VMEM((HP, keys), F32),
            pltpu.SemaphoreType.DMA((n,)),
            pltpu.SemaphoreType.DMA((n,)),
            pltpu.SemaphoreType.DMA((n,)),
            pltpu.SemaphoreType.DMA,
            pltpu.SemaphoreType.DMA((len(args),)),
            pltpu.VMEM((rows * HP, keys), F32),
            pltpu.VMEM((rows * HP, keys), F32),
        ],
        compiler_params=pltpu.CompilerParams(
            collective_id=0, has_side_effects=True, vmem_limit_bytes=67043328
        ),
    )(*args)


def solution(mesh):
    row = P("blk", None)
    col = P(None, "blk")
    in_specs = (row, col, col, row, row, P("blk"), P("blk")) + (P(),) * 12
    return jax.shard_map(
        functools.partial(per_device, mesh.shape["blk"]),
        mesh=mesh, in_specs=in_specs, out_specs=(row, col), check_vma=False,
    )
```
